32 devices in a mesh: dp: 1 (over z), tp: 4 (over y), pp: 8 (over x, core).
Axes of the slice: x: 4, y: 4, z: 1, core: 2. Of those that a mesh axis runs over, the one named last changes fastest.
The devices are a block of a 4x4x8 slice.
Arguments:
- stage_buf: bfloat16 [8, 16, 512, 1024], P('pp', 'dp', 'tp')
- new_mb: bfloat16 [16, 512, 1024], P('dp', 'tp')
- positions: int32 [512], replicated
- ln_attn: float32 [8, 2, 1024], P('pp')
- ln_mlp: float32 [8, 2, 1024], P('pp')
- w_qkv: bfloat16 [8, 16, 3, 64, 1024], P('pp', 'tp')
- w_out: bfloat16 [8, 1024, 1024], P('pp', 'tp')
- w_up: bfloat16 [8, 1024, 4096], P('pp', None, 'tp')
- w_down: bfloat16 [8, 4096, 1024], P('pp', 'tp')
Outputs:
- output 1: bfloat16 [16, 512, 1024], P('dp', 'tp', 'pp')
- output 2: bfloat16 [16, 512, 1024], P('dp', 'tp', 'pp')
- output 3: bfloat16 [8, 16, 512, 1024], P('pp', 'dp', 'tp')
All inputs are finite; a program needn't handle non-finite values.
Results may differ from the reference program's by a relative error of at most 0.0179908.
Values are sent between devices in bfloat16 or wider.
A program may use at most 768 MiB of HBM per device.

```python
import jax
import jax.numpy as jnp
from jax import lax

STAGES = 8
MICRO_BATCH = 16
SEQ_LEN = 512
D_MODEL = 1024
N_HEADS = 16
KV_GROUPS = 16
HEAD_DIM = 64
FF_DIM = 4096
LN_EPS = 1e-5
ROPE_BASE = 10000.0


def setup_inputs(seed: int = 0, part: int = 0) -> dict:
    base_key = jax.random.key(seed)
    key_list = jax.random.split(base_key, 8)
    act_keys = jax.random.split(jax.random.fold_in(key_list[7], part), 2)
    groups = N_HEADS // KV_GROUPS
    in_scale = D_MODEL ** -0.5
    stage_buf = jax.random.normal(act_keys[0], (STAGES, MICRO_BATCH, SEQ_LEN, D_MODEL), jnp.float32).astype(jnp.bfloat16)
    new_mb = jax.random.normal(act_keys[1], (MICRO_BATCH, SEQ_LEN, D_MODEL), jnp.float32).astype(jnp.bfloat16)
    pos_steps = jax.random.randint(key_list[0], (SEQ_LEN,), 1, 4)
    offset = jax.random.randint(key_list[1], (), 0, SEQ_LEN)
    positions = (offset + jnp.cumsum(pos_steps) - 1).astype(jnp.int32)
    ln_noise = 0.2 * jax.random.normal(key_list[2], (2, STAGES, 2, D_MODEL), jnp.float32)
    ln_base = jnp.array([1.0, 0.0], jnp.float32)[None, :, None]
    w_qkv = (1.5 * in_scale * jax.random.normal(key_list[3], (STAGES, KV_GROUPS, groups + 2, HEAD_DIM, D_MODEL), jnp.float32)).astype(jnp.bfloat16)
    w_out = (in_scale * jax.random.normal(key_list[4], (STAGES, D_MODEL, D_MODEL), jnp.float32)).astype(jnp.bfloat16)
    w_up = (in_scale * jax.random.normal(key_list[5], (STAGES, D_MODEL, FF_DIM), jnp.float32)).astype(jnp.bfloat16)
    w_down = (FF_DIM ** -0.5 * jax.random.normal(key_list[6], (STAGES, FF_DIM, D_MODEL), jnp.float32)).astype(jnp.bfloat16)
    return {"stage_buf": stage_buf, "new_mb": new_mb, "positions": positions, "ln_attn": ln_base + ln_noise[0], "ln_mlp": ln_base + ln_noise[1], "w_qkv": w_qkv, "w_out": w_out, "w_up": w_up, "w_down": w_down}


def rope_tables(positions):
    inv_freq = 1.0 / (ROPE_BASE ** (jnp.arange(0, HEAD_DIM, 2).astype(jnp.float32) / HEAD_DIM))
    angles = positions.astype(jnp.float32)[:, None] * inv_freq[None, :]
    return jnp.cos(angles), jnp.sin(angles)


def layer_norm(x_in, ln_params):
    x_wide = x_in.astype(jnp.float32)
    centered = x_wide - jnp.mean(x_wide, axis=-1, keepdims=True)
    variance = jnp.mean(jnp.square(centered), axis=-1, keepdims=True)
    return (centered * lax.rsqrt(variance + LN_EPS) * ln_params[0] + ln_params[1]).astype(jnp.bfloat16)


def rotate_half(x_in, cos_tab, sin_tab):
    half_dim = x_in.shape[-1] // 2
    x_wide = x_in.astype(jnp.float32)
    first_half = x_wide[..., :half_dim]
    second_half = x_wide[..., half_dim:]
    return jnp.concatenate([first_half * cos_tab - second_half * sin_tab, second_half * cos_tab + first_half * sin_tab], axis=-1).astype(jnp.bfloat16)


def apply_layer(x_in, ln_attn, ln_mlp, w_qkv, w_out, w_up, w_down, cos_tab, sin_tab):
    groups = N_HEADS // KV_GROUPS
    a_norm = layer_norm(x_in, ln_attn).reshape(MICRO_BATCH * SEQ_LEN, D_MODEL)
    m_norm = layer_norm(x_in, ln_mlp).reshape(MICRO_BATCH * SEQ_LEN, D_MODEL)
    qkv_proj = jnp.dot(a_norm, w_qkv.reshape(-1, D_MODEL).T, preferred_element_type=jnp.float32).astype(jnp.bfloat16)
    qkv_proj = qkv_proj.reshape(MICRO_BATCH, SEQ_LEN, KV_GROUPS, groups + 2, HEAD_DIM)
    queries = rotate_half(qkv_proj[:, :, :, :groups], cos_tab[:, None, None], sin_tab[:, None, None])
    key_rot = rotate_half(qkv_proj[:, :, :, groups], cos_tab[:, None], sin_tab[:, None])
    values = qkv_proj[:, :, :, groups + 1]
    scores = jnp.einsum("bskgh,btkh->bkgst", queries.astype(jnp.float32), key_rot.astype(jnp.float32)) * HEAD_DIM ** -0.5
    causal = jnp.arange(SEQ_LEN)[:, None] >= jnp.arange(SEQ_LEN)[None, :]
    attn_probs = jax.nn.softmax(jnp.where(causal, scores, -1e30), axis=-1).astype(jnp.bfloat16)
    attn_heads = jnp.einsum("bkgst,btkh->bskgh", attn_probs.astype(jnp.float32), values.astype(jnp.float32)).astype(jnp.bfloat16)
    attn_part = jnp.dot(attn_heads.reshape(MICRO_BATCH * SEQ_LEN, D_MODEL), w_out, preferred_element_type=jnp.float32)
    hidden = jax.nn.gelu(jnp.dot(m_norm, w_up, preferred_element_type=jnp.float32), approximate=False).astype(jnp.bfloat16)
    mlp_part = jnp.dot(hidden, w_down, preferred_element_type=jnp.float32)
    summed = x_in.astype(jnp.float32) + (attn_part + mlp_part).reshape(MICRO_BATCH, SEQ_LEN, D_MODEL)
    return summed.astype(jnp.bfloat16)


def reference(stage_buf, new_mb, positions, ln_attn, ln_mlp, w_qkv, w_out, w_up, w_down):
    cos_tab, sin_tab = rope_tables(positions)

    def layer_step(stage_item):
        return apply_layer(stage_item[0], stage_item[1], stage_item[2], stage_item[3], stage_item[4], stage_item[5], stage_item[6], cos_tab, sin_tab)

    def run_tick(stage_bufs):
        return lax.map(layer_step, (stage_bufs, ln_attn, ln_mlp, w_qkv, w_out, w_up, w_down))

    out_one = run_tick(stage_buf)
    buf_one = jnp.concatenate([new_mb[None], out_one[:-1]], axis=0)
    out_two = run_tick(buf_one)
    final_buf = jnp.concatenate([jnp.zeros_like(new_mb)[None], out_two[:-1]], axis=0)
    return (out_one[-1], out_two[-1], final_buf)
```

```python
import functools
import math

import jax
import jax.numpy as jnp
from jax import lax
from jax.experimental import pallas as pl
from jax.experimental.pallas import tpu as pltpu
from jax.sharding import PartitionSpec as P

LN_EPS = 1e-5
ROPE_BASE = 10000.0
F32 = jnp.float32
BF16 = jnp.bfloat16


def nt_dot(lhs, rhs):
    return lax.dot_general(lhs, rhs, (((1,), (1,)), ((), ())), preferred_element_type=F32)


def nn_dot(lhs, rhs):
    return jnp.dot(lhs, rhs, preferred_element_type=F32)


def rows_kernel(dims, pieces, first, last, *refs):
    seq, width, heads, head_dim, ff = dims
    qk_w = heads * head_dim
    half_w = qk_w // 2
    qkv_rows = 3 * qk_w
    n_slots = len(pieces)
    n_src = sum(len(slot) for slot in pieces)
    refs = list(refs)
    x_ref = refs.pop(0)
    acc_ref = None if first else refs.pop(0)
    ln_ref, cos_ref, sin_ref = refs[:3]
    srcs = refs[3:3 + n_src]
    out_ref, wbuf, a_s, m_s, q_s, k_s, v_s, km_s, vm_s, o_s, h_s, acc_s, sem = refs[3 + n_src:]

    def copies(slot):
        base = sum(len(s) for s in pieces[:slot])
        row = 0
        found = []
        for i, rows in enumerate(pieces[slot]):
            found.append(pltpu.make_async_copy(srcs[base + i], wbuf.at[slot % 2, pl.ds(row, rows)], sem.at[slot % 2]))
            row += rows
        return found

    def start_slot(slot):
        for copy in copies(slot):
            copy.start()

    def wait_slot(buf):
        pltpu.make_async_copy(wbuf.at[buf], wbuf.at[buf], sem.at[buf]).wait()

    if n_slots == 1:
        @pl.when(pl.program_id(0) == 0)
        def _():
            start_slot(0)
    else:
        start_slot(0)

    ln_rows = 64

    def norm_body(i, carry):
        rows = pl.ds(pl.multiple_of(i * ln_rows, ln_rows), ln_rows)
        wide = x_ref[0, rows, :].astype(F32)
        if first:
            acc_s[rows, :] = wide
        else:
            acc_s[rows, :] = acc_ref[0, rows, :]
        centered = wide - jnp.mean(wide, axis=-1, keepdims=True)
        var = jnp.mean(jnp.square(centered), axis=-1, keepdims=True)
        normed = centered * lax.rsqrt(var + LN_EPS)
        a_s[rows, :] = (normed * ln_ref[0:1, :] + ln_ref[1:2, :]).astype(BF16)
        m_s[rows, :] = (normed * ln_ref[2:3, :] + ln_ref[3:4, :]).astype(BF16)
        return carry

    lax.fori_loop(0, seq // ln_rows, norm_body, 0)

    if n_slots == 1:
        @pl.when(pl.program_id(0) == 0)
        def _():
            wait_slot(0)

    exp_scale = math.log2(math.e) * head_dim ** -0.5
    q_blk = 128

    def add_slot(w):
        qkv = nt_dot(a_s[...], w[0:qkv_rows, :])
        qk = qkv[:, :2 * qk_w].astype(BF16).astype(F32)
        cos = cos_ref[...]
        sin = sin_ref[...]
        for dst, lo in ((q_s, 0), (k_s, qk_w)):
            first_half = qk[:, lo:lo + half_w]
            second_half = qk[:, lo + half_w:lo + qk_w]
            dst[:, :half_w] = (first_half * cos - second_half * sin).astype(BF16)
            dst[:, half_w:] = (second_half * cos + first_half * sin).astype(BF16)
        v_s[...] = qkv[:, 2 * qk_w:].astype(BF16)
        o_s[...] = jnp.zeros_like(o_s)

        lane = lax.broadcasted_iota(jnp.int32, (seq, qk_w), 1)
        causal = lax.broadcasted_iota(jnp.int32, (q_blk, q_blk), 0) >= lax.broadcasted_iota(jnp.int32, (q_blk, q_blk), 1)

        def head_body(h, carry):
            km_s[...] = jnp.where((lane % half_w) // (head_dim // 2) == h, k_s[...], jnp.zeros((), BF16))
            vm_s[...] = jnp.where(lane // head_dim == h, v_s[...], jnp.zeros((), BF16))
            for blk in range(seq // q_blk):
                lo = blk * q_blk
                hi = lo + q_blk
                s_diag = jnp.where(causal, nt_dot(q_s[lo:hi, :], km_s[lo:hi, :]), -1e30)
                top = jnp.max(s_diag, axis=-1, keepdims=True)
                if blk:
                    s_past = nt_dot(q_s[lo:hi, :], km_s[0:lo, :])
                    top = jnp.maximum(top, jnp.max(s_past, axis=-1, keepdims=True))
                e_diag = jnp.exp2((s_diag - top) * exp_scale)
                tot = jnp.sum(e_diag, axis=-1, keepdims=True)
                if blk:
                    e_past = jnp.exp2((s_past - top) * exp_scale)
                    tot = tot + jnp.sum(e_past, axis=-1, keepdims=True)
                inv = 1.0 / tot
                o_blk = nn_dot((e_diag * inv).astype(BF16), vm_s[lo:hi, :])
                if blk:
                    o_blk = o_blk + nn_dot((e_past * inv).astype(BF16), vm_s[0:lo, :])
                o_s[lo:hi, :] += o_blk
            return carry

        lax.fori_loop(0, heads, head_body, 0)
        h_s[:, 0:qk_w] = o_s[...].astype(BF16)

        col = 256
        up0 = qkv_rows
        for j in range(ff // col):
            pre = nn_dot(m_s[...], w[up0:up0 + width, j * col:(j + 1) * col])
            act = 0.5 * pre * (1.0 + lax.erf(pre * math.sqrt(0.5)))
            h_s[:, qk_w + j * col:qk_w + (j + 1) * col] = act.astype(BF16)
        out0 = up0 + width
        for j in range(width // col):
            acc_s[:, j * col:(j + 1) * col] += nn_dot(h_s[...], w[out0:out0 + qk_w + ff, j * col:(j + 1) * col])

    if n_slots == 1:
        add_slot(wbuf.at[0])
    else:
        def slot_body(slot, carry):
            for i in range(1, n_slots):
                @pl.when(slot + 1 == i)
                def _(i=i):
                    start_slot(i)
            buf = lax.rem(slot, 2)
            wait_slot(buf)
            add_slot(wbuf.at[buf])
            return carry

        lax.fori_loop(0, n_slots, slot_body, 0)
    if last:
        out_ref[0] = acc_s[...].astype(BF16)
    else:
        out_ref[0] = acc_s[...]


def run_rows(dims, x_rows, acc, lns, cos_tab, sin_tab, slots, last, span=None):
    seq, width, heads, head_dim, ff = dims
    row0, row1 = span or (0, x_rows.shape[0])
    rows = row1 - row0
    qk_w = heads * head_dim
    w_rows = 3 * qk_w + width + qk_w + ff
    n_buf = 1 if len(slots) == 1 else 2
    pieces = [[piece.shape[0] for piece in slot] for slot in slots]
    flat = [piece for slot in slots for piece in slot]
    first = acc is None
    row_spec = pl.BlockSpec((1, seq, width), lambda i: (row0 + i, 0, 0))
    out_spec = pl.BlockSpec((1, seq, width), lambda i: (i, 0, 0))
    fixed = lambda arr: pl.BlockSpec(arr.shape, lambda i: (0,) * arr.ndim)
    operands = [x_rows] + ([] if first else [acc]) + [lns, cos_tab, sin_tab] + flat
    specs = [row_spec] + ([] if first else [row_spec]) + [fixed(lns), fixed(cos_tab), fixed(sin_tab)]
    specs += [pl.BlockSpec(memory_space=pltpu.HBM)] * len(flat)
    flops = 2 * rows * seq * width * (3 * qk_w + qk_w + 2 * ff) * len(slots)
    return pl.pallas_call(
        functools.partial(rows_kernel, dims, pieces, first, last),
        grid=(rows,),
        out_shape=jax.ShapeDtypeStruct((rows, seq, width), BF16 if last else F32),
        in_specs=specs,
        out_specs=out_spec,
        scratch_shapes=[
            pltpu.VMEM((n_buf, w_rows, width), BF16),
            pltpu.VMEM((seq, width), BF16),
            pltpu.VMEM((seq, width), BF16),
            pltpu.VMEM((seq, qk_w), BF16),
            pltpu.VMEM((seq, qk_w), BF16),
            pltpu.VMEM((seq, qk_w), BF16),
            pltpu.VMEM((seq, qk_w), BF16),
            pltpu.VMEM((seq, qk_w), BF16),
            pltpu.VMEM((seq, qk_w), F32),
            pltpu.VMEM((seq, qk_w + ff), BF16),
            pltpu.VMEM((seq, width), F32),
            pltpu.SemaphoreType.DMA((n_buf,)),
        ],
        compiler_params=pltpu.CompilerParams(dimension_semantics=("arbitrary",), vmem_limit_bytes=52 * 1024 * 1024),
        cost_estimate=pl.CostEstimate(flops=flops, bytes_accessed=len(slots) * w_rows * width * 2, transcendentals=0),
    )(*operands)


def rope_tables(positions, head_dim, heads):
    inv_freq = 1.0 / (ROPE_BASE ** (jnp.arange(0, head_dim, 2).astype(F32) / head_dim))
    angles = positions.astype(F32)[:, None] * inv_freq[None, :]
    return jnp.tile(jnp.cos(angles), (1, heads)), jnp.tile(jnp.sin(angles), (1, heads))


def pack_weights(w_qkv, w_out, w_up, w_down):
    heads, _, head_dim, width = w_qkv.shape
    halves = w_qkv.reshape(heads, 3, 2, head_dim // 2, width)
    qk = halves[:, :2].transpose(1, 2, 0, 3, 4).reshape(-1, width)
    values = w_qkv[:, 2].reshape(-1, width)
    return jnp.concatenate([qk, values, w_up, w_out, w_down], axis=0)


def solution(mesh):
    stages = mesh.shape["pp"]
    ranks = mesh.shape["tp"]
    both = ("tp", "pp")
    run = run_rows

    def stage_body(stage_buf, new_mb, positions, ln_attn, ln_mlp, w_qkv, w_out, w_up, w_down):
        rank = lax.axis_index("tp")
        stage = lax.axis_index("pp")
        mb, seq_loc, width = new_mb.shape
        seq = seq_loc * ranks
        blk = mb // ranks
        heads, head_dim = w_qkv.shape[1], w_qkv.shape[3]
        ff = w_up.shape[2]
        dims = (seq, width, heads, head_dim, ff)
        cos_tab, sin_tab = rope_tables(positions, head_dim, heads)
        lns = jnp.concatenate([ln_attn[0], ln_mlp[0]], axis=0)

        def dev(t, p):
            return (t % ranks) * stages + p

        def ring(arr, step, only=None):
            group = range(stages) if only is None else only
            return lax.ppermute(arr, both, [(dev(t, p), dev(t + step, p)) for t in range(ranks) for p in group])

        def to_rows(shard, only=None):
            full = jnp.zeros((blk, seq, width), BF16)
            for k in range(ranks):
                part = lax.dynamic_slice_in_dim(shard, blk * ((rank + k) % ranks), blk, axis=0)
                if k:
                    part = ring(part, k, only)
                full = lax.dynamic_update_slice_in_dim(full, part, seq_loc * ((rank - k) % ranks), axis=1)
            return full

        own = pack_weights(w_qkv[0], w_out[0], w_up[0], w_down[0])
        half = own.shape[0] // 2
        x_rows = to_rows(stage_buf[0])
        from_left = ring(own, 1)
        from_right = ring(own, -1)
        far_top = ring(from_left[:half], 1)
        far_bottom = ring(from_right[half:], -1)
        slots = [[own], [from_left], [from_right], [far_top, far_bottom]]

        acc = run(dims, x_rows, None, lns, cos_tab, sin_tab, slots[:1], False)
        acc = run(dims, x_rows, acc, lns, cos_tab, sin_tab, slots[1:2], False)
        acc = run(dims, x_rows, acc, lns, cos_tab, sin_tab, slots[2:3], False)
        late_mb, _ = lax.optimization_barrier((new_mb, far_top[:8, :128]))
        mb_rows = to_rows(late_mb, only=[0])
        next_stage = [(dev(t, p), dev(t, p + 1)) for t in range(ranks) for p in range(stages - 1)]
        y_one, x_two = [], []
        for i in range(blk):
            y_row = run(dims, x_rows, acc, lns, cos_tab, sin_tab, slots[3:], True, (i, i + 1))
            y_one.append(y_row)
            x_two.append(lax.ppermute(y_row, both, next_stage))

        cols = width // stages

        def spread(part):
            reach = stages // 2
            while reach:
                mid = part.shape[-1] // 2
                send = [(dev(t, p), dev(t, p - reach)) for t in range(ranks) for p in range(stages - 1, -1, -2 * reach)]
                got = lax.ppermute(part[..., :mid], both, send)
                part = jnp.where((stage // reach) % 2 == 1, part[..., mid:], got)
                reach //= 2
            return part

        emit_parts = [spread(jnp.concatenate(y_one, axis=0))]
        final_buf = jnp.zeros((mb, seq_loc, width), BF16)
        y_two = []
        groups = {1: (0, 2), 2: (2, 3), 3: (3, 4)}
        emits = {2: (0, 3), 3: (3, 4)}
        for i in range(blk):
            got = x_two[i]
            if i:
                got, y_two[-1] = lax.optimization_barrier((got, y_two[-1]))
            x_row = jnp.where(stage == 0, mb_rows[i:i + 1], got)
            y_two.append(run(dims, x_row, None, lns, cos_tab, sin_tab, slots, True))
            if i in groups:
                lo, hi = groups[i]
                group = jnp.concatenate(y_two[lo:hi], axis=0)
                for k in range(ranks):
                    part = lax.dynamic_slice_in_dim(group, seq_loc * ((rank + k) % ranks), seq_loc, axis=1)
                    part = lax.ppermute(part, both, [(dev(t, p), dev(t + k, p + 1)) for t in range(ranks) for p in range(stages - 1)])
                    final_buf = lax.dynamic_update_slice_in_dim(final_buf, part, blk * ((rank - k) % ranks) + lo, axis=0)
            if i in emits:
                lo, hi = emits[i]
                emit_parts.append(spread(jnp.concatenate(y_two[lo:hi], axis=0)))

        emit_rows = jnp.concatenate(emit_parts, axis=0).reshape(2, blk, seq, cols)
        emit = jnp.zeros((2, mb, seq_loc, cols), BF16)
        for k in range(ranks):
            part = lax.dynamic_slice_in_dim(emit_rows, seq_loc * ((rank + k) % ranks), seq_loc, axis=2)
            if k:
                part = ring(part, k)
            emit = lax.dynamic_update_slice_in_dim(emit, part, blk * ((rank - k) % ranks), axis=1)
        return emit[0], emit[1], final_buf[None]

    act_spec = P("dp", "tp", None)
    buf_spec = P("pp", "dp", "tp", None)
    emit_spec = P("dp", "tp", "pp")
    stack_spec = P("pp", None, None)
    return jax.shard_map(stage_body, mesh=mesh, in_specs=(buf_spec, act_spec, P(None), stack_spec, stack_spec, P("pp", "tp", None, None, None), P("pp", "tp", None), P("pp", None, "tp"), P("pp", "tp", None)), out_specs=(emit_spec, emit_spec, buf_spec), check_vma=False)
```

```python
import functools
import math

import jax
import jax.numpy as jnp
from jax import lax
from jax.experimental import pallas as pl
from jax.experimental.pallas import tpu as pltpu
from jax.sharding import PartitionSpec as P

LN_EPS = 1e-5
ROPE_BASE = 10000.0
F32 = jnp.float32
BF16 = jnp.bfloat16
MESH = pl.DeviceIdType.MESH
LN_ROWS = 64
Q_BLK = 128
COL = 256


def nt_dot(lhs, rhs):
    return lax.dot_general(lhs, rhs, (((1,), (1,)), ((), ())), preferred_element_type=F32)


def nn_dot(lhs, rhs):
    return jnp.dot(lhs, rhs, preferred_element_type=F32)


def gelu(pre):
    return 0.5 * pre * (1.0 + lax.erf(pre * math.sqrt(0.5)))


def normalise(dims, x_ref, acc_ref, a_ref, m_ref, ln_ref):
    def body(i, carry):
        rows = pl.ds(pl.multiple_of(i * LN_ROWS, LN_ROWS), LN_ROWS)
        wide = x_ref[rows, :].astype(F32)
        acc_ref[rows, :] = wide
        centered = wide - jnp.mean(wide, axis=-1, keepdims=True)
        var = jnp.mean(jnp.square(centered), axis=-1, keepdims=True)
        normed = centered * lax.rsqrt(var + LN_EPS)
        a_ref[rows, :] = (normed * ln_ref[0:1, :] + ln_ref[1:2, :]).astype(BF16)
        m_ref[rows, :] = (normed * ln_ref[2:3, :] + ln_ref[3:4, :]).astype(BF16)
        return carry

    lax.fori_loop(0, dims[0] // LN_ROWS, body, 0)


def add_quarter(dims, a_ref, m_ref, w, acc_ref, cos_ref, sin_ref, q_s, k_s, v_s, km_s, vm_s, o_s, h_s):
    seq, width, heads, head_dim, ff = dims
    qk_w = heads * head_dim
    half_w = qk_w // 2
    qkv_rows = 3 * qk_w
    qkv = nt_dot(a_ref[...], w[0:qkv_rows, :])
    qk = qkv[:, :2 * qk_w].astype(BF16).astype(F32)
    cos = cos_ref[...]
    sin = sin_ref[...]
    for dst, lo in ((q_s, 0), (k_s, qk_w)):
        first_half = qk[:, lo:lo + half_w]
        second_half = qk[:, lo + half_w:lo + qk_w]
        dst[:, :half_w] = (first_half * cos - second_half * sin).astype(BF16)
        dst[:, half_w:] = (second_half * cos + first_half * sin).astype(BF16)
    v_s[...] = qkv[:, 2 * qk_w:].astype(BF16)
    o_s[...] = jnp.zeros_like(o_s)

    exp_scale = math.log2(math.e) * head_dim ** -0.5
    lane = lax.broadcasted_iota(jnp.int32, (1, qk_w), 1)
    key_head = (lane % half_w) // (head_dim // 2)
    value_head = lane // head_dim
    causal = lax.broadcasted_iota(jnp.int32, (Q_BLK, Q_BLK), 0) >= lax.broadcasted_iota(jnp.int32, (Q_BLK, Q_BLK), 1)

    def head_body(h, carry):
        km_s[...] = k_s[...] * jnp.where(key_head == h, 1.0, 0.0).astype(BF16)
        vm_s[...] = v_s[...] * jnp.where(value_head == h, 1.0, 0.0).astype(BF16)
        for blk in range(seq // Q_BLK):
            lo = blk * Q_BLK
            hi = lo + Q_BLK
            s_diag = jnp.where(causal, nt_dot(q_s[lo:hi, :], km_s[lo:hi, :]), -1e30)
            top = jnp.max(s_diag, axis=-1, keepdims=True)
            if blk:
                s_past = nt_dot(q_s[lo:hi, :], km_s[0:lo, :])
                top = jnp.maximum(top, jnp.max(s_past, axis=-1, keepdims=True))
            e_diag = jnp.exp2((s_diag - top) * exp_scale)
            tot = jnp.sum(e_diag, axis=-1, keepdims=True)
            if blk:
                e_past = jnp.exp2((s_past - top) * exp_scale)
                tot = tot + jnp.sum(e_past, axis=-1, keepdims=True)
            inv = 1.0 / tot
            o_blk = nn_dot((e_diag * inv).astype(BF16), vm_s[lo:hi, :])
            if blk:
                o_blk = o_blk + nn_dot((e_past * inv).astype(BF16), vm_s[0:lo, :])
            o_s[lo:hi, :] += o_blk
        return carry

    lax.fori_loop(0, heads, head_body, 0)
    h_s[:, 0:qk_w] = o_s[...].astype(BF16)

    for j in range(ff // COL):
        pre = nn_dot(m_ref[...], w[qkv_rows:qkv_rows + width, j * COL:(j + 1) * COL])
        h_s[:, qk_w + j * COL:qk_w + (j + 1) * COL] = gelu(pre).astype(BF16)
    out0 = qkv_rows + width
    for j in range(width // COL):
        acc_ref[:, j * COL:(j + 1) * COL] += nn_dot(h_s[...], w[out0:out0 + qk_w + ff, j * COL:(j + 1) * COL])


def ticks_kernel(dims, ranks, stages, stage_ref, mb_ref, own_ref, ln_ref, cos_ref, sin_ref, emit_one, emit_two, final_ref,
                 wbuf, xs, acc, a_s, m_s, q_s, k_s, v_s, km_s, vm_s, o_s, h_s, zero_s,
                 x_send, x_recv, mb_send, w_send, w_recv, y_send, out_send, out_recv):
    seq, width = dims[:2]
    seq_loc = seq // ranks
    blk = xs.shape[1]
    cols = width // stages
    half = wbuf.shape[1] // 2
    y = lax.axis_index("tp")
    p = lax.axis_index("pp")
    chip = p // 2
    core = p % 2
    role = (y // 2 + chip) % 2
    layer = 2 * chip + role
    last = layer == stages - 1
    home = core == role
    sibling = p + 1 - 2 * core
    mate = y + 1 - 2 * (y % 2)
    across = ranks - 1 - y
    block_one = 2 * (y % 2) + core
    block_two = jnp.where(role == 0, block_one, 2 * (1 - y % 2) + core)
    my_seq = pl.ds(pl.multiple_of(y * seq_loc, seq_loc), seq_loc)
    my_half = pl.ds(pl.multiple_of(core * half, half), half)

    def remote(src, dst, send, recv, tp, pp):
        return pltpu.make_async_remote_copy(src_ref=src, dst_ref=dst, send_sem=send, recv_sem=recv, device_id={"tp": tp, "pp": pp}, device_id_type=MESH)

    def put(src, dst, send, recv, tp, pp):
        here = jnp.logical_and(tp == y, pp == p)

        @pl.when(here)
        def _():
            pltpu.make_async_copy(src, dst, recv).start()

        @pl.when(jnp.logical_not(here))
        def _():
            remote(src, dst, send, recv, tp, pp).start()

    def wait_bytes(like, sem):
        pltpu.make_async_copy(like, like, sem).wait()

    own_copy = pltpu.make_async_copy(own_ref, wbuf.at[0], w_recv.at[0])
    own_send = remote(own_ref, wbuf.at[0], w_send.at[0], w_recv.at[0], y, sibling)

    @pl.when(home)
    def _():
        own_copy.start()
        own_send.start()

    pair_of_stage = (core + chip) % 2

    def send_x(i, carry):
        for b in range(ranks):
            put(stage_ref.at[b * blk + i], xs.at[0, i, my_seq], x_send, x_recv.at[0, i], 2 * pair_of_stage + b // 2, 2 * chip + b % 2)
        return carry

    lax.fori_loop(0, blk, send_x, 0)

    @pl.when(home)
    def _():
        for h in range(2):
            part = pl.ds(h * half, half)
            remote(own_ref.at[part], wbuf.at[1, part], w_send.at[1], w_recv.at[1], mate, 2 * chip + h).start()

    @pl.when(jnp.logical_not(home))
    def _():
        for h in range(2):
            part = pl.ds(h * half, half)
            remote(own_ref.at[part], wbuf.at[2, part], w_send.at[1], w_recv.at[3], across, 2 * chip + h).start()

    @pl.when(p == 0)
    def _():
        zero_s[...] = jnp.zeros_like(zero_s)

        def put_zero(n, carry):
            pltpu.make_async_copy(zero_s, final_ref.at[n], out_recv.at[0]).start()
            return carry

        lax.fori_loop(0, blk * ranks, put_zero, 0)

    mate_swap = [remote(wbuf.at[slot, my_half], wbuf.at[slot, my_half], w_send.at[1 + slot], w_recv.at[2 * slot], y, sibling) for slot in range(1, 4)]
    pass_on = remote(wbuf.at[2, my_half], wbuf.at[3, my_half], w_send.at[5], w_recv.at[5], mate, p)

    def before_slot(slot):
        if slot == 0:
            wait_bytes(wbuf.at[0], w_recv.at[0])
        elif slot == 1:
            wait_bytes(wbuf.at[2, my_half], w_recv.at[3])
            pass_on.start()
            mate_swap[1].start()
            wait_bytes(wbuf.at[1, my_half], w_recv.at[1])
            mate_swap[0].start()

            @pl.when(chip == 0)
            def _():
                def send_mb(i, carry):
                    for b in range(ranks // 2):
                        put(mb_ref.at[(2 * b + core) * blk + i], xs.at[1, i, my_seq], mb_send, x_recv.at[1, i], b, core)
                    return carry

                lax.fori_loop(0, blk, send_mb, 0)

            wait_bytes(wbuf.at[1, my_half], w_recv.at[2])
        elif slot == 2:
            wait_bytes(wbuf.at[2, my_half], w_recv.at[4])
        else:
            wait_bytes(wbuf.at[3, my_half], w_recv.at[5])
            mate_swap[2].start()
            wait_bytes(wbuf.at[3, my_half], w_recv.at[6])

    def send_emit(tick, dst, rows, row0, block):
        def body(n, carry):
            tp, pp = n // stages, n % stages
            src = xs.at[tick, pl.ds(row0, rows), pl.ds(pl.multiple_of(tp * seq_loc, seq_loc), seq_loc), pl.ds(pl.multiple_of(pp * cols, cols), cols)]
            put(src, dst.at[pl.ds(block * blk + row0, rows)], out_send, out_recv.at[1 + tick], tp, pp)
            return carry

        lax.fori_loop(0, ranks * stages, body, 0)

    steps = blk * ranks

    def step_body(step, carry):
        tick = step // steps
        index = step % steps
        slot = jnp.where(tick == 0, index // blk, index % ranks)
        row = jnp.where(tick == 0, index % blk, index // ranks)
        for s in range(ranks):
            @pl.when(step == s * blk)
            def _(s=s):
                before_slot(s)

        @pl.when(slot == 0)
        def _():
            wait_bytes(xs.at[tick, row], x_recv.at[tick, row])
            normalise(dims, xs.at[tick, row], acc.at[row], a_s.at[row], m_s.at[row], ln_ref)

        add_quarter(dims, a_s.at[row], m_s.at[row], wbuf.at[slot], acc.at[row], cos_ref, sin_ref, q_s, k_s, v_s, km_s, vm_s, o_s, h_s)

        @pl.when(slot == ranks - 1)
        def _():
            xs[tick, row] = acc[row].astype(BF16)

            @pl.when(jnp.logical_and(tick == 0, jnp.logical_not(last)))
            def _():
                next_y = jnp.where(role == 0, across, y)
                next_p = jnp.where(role == 0, p, p + 2)
                remote(xs.at[0, row], xs.at[1, row], y_send, x_recv.at[1, row], next_y, next_p).start()

            @pl.when(jnp.logical_and(step == steps - 1, last))
            def _():
                send_emit(0, emit_one, blk, 0, block_one)

            @pl.when(jnp.logical_and(tick == 1, last))
            def _():
                send_emit(1, emit_two, 1, row, block_two)

            @pl.when(jnp.logical_and(tick == 1, jnp.logical_not(last)))
            def _():
                def send_final(n, carry):
                    part = pl.ds(pl.multiple_of(n * seq_loc, seq_loc), seq_loc)
                    put(xs.at[1, row, part], final_ref.at[block_two * blk + row], out_send, out_recv.at[0], n, layer + 1)
                    return carry

                lax.fori_loop(0, ranks, send_final, 0)

        return carry

    lax.fori_loop(0, 2 * steps, step_body, 0)

    wait_bytes(stage_ref.at[pl.ds(0, (ranks - 1) * blk)], x_send)

    @pl.when(home)
    def _():
        wait_bytes(own_ref, w_send.at[0])

    @pl.when(jnp.logical_not(home))
    def _():
        wait_bytes(stage_ref.at[pl.ds(0, blk)], x_send)

    wait_bytes(own_ref, w_send.at[1])
    for slot in range(2, 6):
        wait_bytes(wbuf.at[1, my_half], w_send.at[slot])

    @pl.when(chip == 0)
    def _():
        wait_bytes(mb_ref.at[pl.ds(0, blk)], mb_send)

        @pl.when(role == 1)
        def _():
            wait_bytes(mb_ref.at[pl.ds(0, blk)], mb_send)

    @pl.when(jnp.logical_not(last))
    def _():
        wait_bytes(xs.at[0], y_send)
        wait_bytes(xs.at[1, :, pl.ds(0, seq - seq_loc)], out_send)

        @pl.when(p != layer + 1)
        def _():
            wait_bytes(xs.at[1, :, pl.ds(0, seq_loc)], out_send)

    @pl.when(last)
    def _():
        wait_bytes(xs.at[:, :, pl.ds(0, seq - seq_loc)], out_send)
        wait_bytes(xs.at[:, :, pl.ds(0, seq_loc), pl.ds(0, width - cols)], out_send)

    wait_bytes(final_ref, out_recv.at[0])
    wait_bytes(emit_one, out_recv.at[1])
    wait_bytes(emit_two, out_recv.at[2])


def rope_tables(positions, head_dim, heads):
    inv_freq = 1.0 / (ROPE_BASE ** (jnp.arange(0, head_dim, 2).astype(F32) / head_dim))
    angles = positions.astype(F32)[:, None] * inv_freq[None, :]
    return jnp.tile(jnp.cos(angles), (1, heads)), jnp.tile(jnp.sin(angles), (1, heads))


def pack_weights(w_qkv, w_out, w_up, w_down):
    heads, _, head_dim, width = w_qkv.shape
    halves = w_qkv.reshape(heads, 3, 2, head_dim // 2, width)
    qk = halves[:, :2].transpose(1, 2, 0, 3, 4).reshape(-1, width)
    values = w_qkv[:, 2].reshape(-1, width)
    return jnp.concatenate([qk, values, w_up, w_out, w_down], axis=0)


def solution(mesh):
    stages = mesh.shape["pp"]
    ranks = mesh.shape["tp"]

    def stage_body(stage_buf, new_mb, positions, ln_attn, ln_mlp, w_qkv, w_out, w_up, w_down):
        mb, seq_loc, width = new_mb.shape
        seq = seq_loc * ranks
        blk = mb // ranks
        heads, head_dim = w_qkv.shape[1], w_qkv.shape[3]
        ff = w_up.shape[2]
        dims = (seq, width, heads, head_dim, ff)
        qk_w = heads * head_dim
        cos_tab, sin_tab = rope_tables(positions, head_dim, heads)
        lns = jnp.concatenate([ln_attn[0], ln_mlp[0]], axis=0)
        stage = lax.axis_index("pp")
        role = (lax.axis_index("tp") // 2 + stage // 2) % 2
        other = lax.ppermute(lns, "pp", [(s, s + 1 - 2 * (s % 2)) for s in range(stages)])
        lns = jnp.where(stage % 2 == role, lns, other)
        own = pack_weights(w_qkv[0], w_out[0], w_up[0], w_down[0])
        hbm = pl.BlockSpec(memory_space=pltpu.HBM)
        vmem = pl.BlockSpec(memory_space=pltpu.VMEM)
        dma = pltpu.SemaphoreType.DMA
        emit = jax.ShapeDtypeStruct((mb, seq_loc, width // stages), BF16)
        emit_one, emit_two, final_buf = pl.pallas_call(
            functools.partial(ticks_kernel, dims, ranks, stages),
            out_shape=(emit, emit, jax.ShapeDtypeStruct((mb, seq_loc, width), BF16)),
            in_specs=[hbm, hbm, hbm, vmem, vmem, vmem],
            out_specs=(hbm, hbm, hbm),
            scratch_shapes=[
                pltpu.VMEM((ranks,) + own.shape, BF16),
                pltpu.VMEM((2, blk, seq, width), BF16),
                pltpu.VMEM((blk, seq, width), F32),
                pltpu.VMEM((blk, seq, width), BF16),
                pltpu.VMEM((blk, seq, width), BF16),
                pltpu.VMEM((seq, qk_w), BF16),
                pltpu.VMEM((seq, qk_w), BF16),
                pltpu.VMEM((seq, qk_w), BF16),
                pltpu.VMEM((seq, qk_w), BF16),
                pltpu.VMEM((seq, qk_w), BF16),
                pltpu.VMEM((seq, qk_w), F32),
                pltpu.VMEM((seq, qk_w + ff), BF16),
                pltpu.VMEM((seq_loc, width), BF16),
                dma, dma((2, blk)), dma, dma((6,)), dma((7,)), dma, dma, dma((3,)),
            ],
            compiler_params=pltpu.CompilerParams(has_side_effects=True, vmem_limit_bytes=63 * 1000 * 1024),
        )(stage_buf[0], new_mb, own, lns, cos_tab, sin_tab)
        return emit_one, emit_two, final_buf[None]

    act_spec = P("dp", "tp", None)
    buf_spec = P("pp", "dp", "tp", None)
    emit_spec = P("dp", "tp", "pp")
    stack_spec = P("pp", None, None)
    return jax.shard_map(stage_body, mesh=mesh, in_specs=(buf_spec, act_spec, P(None), stack_spec, stack_spec, P("pp", "tp", None, None, None), P("pp", "tp", None), P("pp", None, "tp"), P("pp", "tp", None)), out_specs=(emit_spec, emit_spec, buf_spec), check_vma=False)
```

```python
import functools
import math

import jax
import jax.numpy as jnp
from jax import lax
from jax.experimental import pallas as pl
from jax.experimental.pallas import tpu as pltpu
from jax.sharding import PartitionSpec as P

LN_EPS = 1e-5
ROPE_BASE = 10000.0
F32 = jnp.float32
BF16 = jnp.bfloat16
MESH = pl.DeviceIdType.MESH
LN_ROWS = 64
Q_BLK = 256
HEAD_UNROLL = 2
COL = 256


def nt_dot(lhs, rhs):
    return lax.dot_general(lhs, rhs, (((1,), (1,)), ((), ())), preferred_element_type=F32)


def nn_dot(lhs, rhs):
    return jnp.dot(lhs, rhs, preferred_element_type=F32)


def tn_dot(lhs, rhs):
    return lax.dot_general(lhs, rhs, (((0,), (0,)), ((), ())), preferred_element_type=F32)


def gelu(pre):
    return 0.5 * pre * (1.0 + lax.erf(pre * math.sqrt(0.5)))


def normalise(dims, x_ref, acc_ref, a_ref, m_ref, ln_ref):
    def body(i, carry):
        rows = pl.ds(pl.multiple_of(i * LN_ROWS, LN_ROWS), LN_ROWS)
        wide = x_ref[rows, :].astype(F32)
        acc_ref[rows, :] = wide
        centered = wide - jnp.mean(wide, axis=-1, keepdims=True)
        var = jnp.mean(jnp.square(centered), axis=-1, keepdims=True)
        normed = centered * lax.rsqrt(var + LN_EPS)
        a_ref[rows, :] = (normed * ln_ref[0, 0:1, :] + ln_ref[0, 1:2, :]).astype(BF16)
        m_ref[rows, :] = (normed * ln_ref[1, 0:1, :] + ln_ref[1, 1:2, :]).astype(BF16)
        return carry

    lax.fori_loop(0, dims[0] // LN_ROWS, body, 0)


def add_quarter(dims, a_ref, m_ref, w, acc_ref, cos_ref, sin_ref, q_s, k_s, v_s, o_s, h_s):
    seq, width, heads, head_dim, ff = dims
    qk_w = heads * head_dim
    qkv_rows = 3 * qk_w
    hd2 = head_dim // 2
    qkv = nt_dot(w[0:qkv_rows, :], a_ref[...]).astype(BF16)
    cos = cos_ref[...]
    sin = sin_ref[...]
    for h in range(heads):
        base = 3 * h * head_dim
        for dst, lo in ((q_s, base), (k_s, base + head_dim)):
            first_half = qkv[lo:lo + hd2].astype(F32)
            second_half = qkv[lo + hd2:lo + head_dim].astype(F32)
            dst[h * head_dim:h * head_dim + hd2, :] = (first_half * cos - second_half * sin).astype(BF16)
            dst[h * head_dim + hd2:(h + 1) * head_dim, :] = (second_half * cos + first_half * sin).astype(BF16)
        v_s[h * head_dim:(h + 1) * head_dim, :] = qkv[base + 2 * head_dim:base + 3 * head_dim]

    exp_scale = math.log2(math.e) * head_dim ** -0.5
    causal = lax.broadcasted_iota(jnp.int32, (Q_BLK, Q_BLK), 0) <= lax.broadcasted_iota(jnp.int32, (Q_BLK, Q_BLK), 1)

    def head_body(h, carry):
        rows = pl.ds(pl.multiple_of(h * head_dim, head_dim), head_dim)
        for blk in range(seq // Q_BLK):
            lo = blk * Q_BLK
            hi = lo + Q_BLK
            query = q_s[rows, lo:hi]
            s_diag = jnp.where(causal, tn_dot(k_s[rows, lo:hi], query), -1e30)
            top = jnp.max(s_diag, axis=0, keepdims=True)
            if blk:
                s_past = tn_dot(k_s[rows, 0:lo], query)
                top = jnp.maximum(top, jnp.max(s_past, axis=0, keepdims=True))
            e_diag = jnp.exp2((s_diag - top) * exp_scale)
            tot = jnp.sum(e_diag, axis=0, keepdims=True)
            if blk:
                e_past = jnp.exp2((s_past - top) * exp_scale)
                tot = tot + jnp.sum(e_past, axis=0, keepdims=True)
            inv = 1.0 / tot
            o_blk = nn_dot(v_s[rows, lo:hi], (e_diag * inv).astype(BF16))
            if blk:
                o_blk = o_blk + nn_dot(v_s[rows, 0:lo], (e_past * inv).astype(BF16))
            o_s[rows, lo:hi] = o_blk
        return carry

    lax.fori_loop(0, heads, head_body, 0, unroll=HEAD_UNROLL)
    h_s[:, 0:qk_w] = jnp.transpose(o_s[...]).astype(BF16)

    for j in range(ff // COL):
        pre = nn_dot(m_ref[...], w[qkv_rows:qkv_rows + width, j * COL:(j + 1) * COL])
        h_s[:, qk_w + j * COL:qk_w + (j + 1) * COL] = gelu(pre).astype(BF16)
    out0 = qkv_rows + width
    for j in range(width // COL):
        acc_ref[:, j * COL:(j + 1) * COL] += nn_dot(h_s[...], w[out0:out0 + qk_w + ff, j * COL:(j + 1) * COL])


def ticks_kernel(dims, ranks, stages, stage_ref, mb_ref, qkv_ref, up_ref, wo_ref, down_ref, ln_attn_ref, ln_mlp_ref, cos_ref, sin_ref,
                 emit_one, emit_two, final_ref, wbuf, xs, acc, a_s, m_s, q_s, k_s, v_s, o_s, h_s, zero_s, ln_s,
                 x_send, x_recv, mb_send, w_send, w_recv, y_send, out_send, out_recv, ln_send, ln_recv):
    seq, width = dims[:2]
    seq_loc = seq // ranks
    blk = xs.shape[1]
    cols = width // stages
    half = wbuf.shape[1] // 2
    y = lax.axis_index("tp")
    p = lax.axis_index("pp")
    chip = p // 2
    core = p % 2
    role = (y // 2 + chip) % 2
    layer = 2 * chip + role
    last = layer == stages - 1
    home = core == role
    sibling = p + 1 - 2 * core
    mate = y + 1 - 2 * (y % 2)
    across = ranks - 1 - y
    block_one = 2 * (y % 2) + core
    block_two = jnp.where(role == 0, block_one, 2 * (1 - y % 2) + core)
    my_seq = pl.ds(pl.multiple_of(y * seq_loc, seq_loc), seq_loc)
    my_half = pl.ds(pl.multiple_of(core * half, half), half)

    def remote(src, dst, send, recv, tp, pp):
        return pltpu.make_async_remote_copy(src_ref=src, dst_ref=dst, send_sem=send, recv_sem=recv, device_id={"tp": tp, "pp": pp}, device_id_type=MESH)

    def put(src, dst, send, recv, tp, pp):
        here = jnp.logical_and(tp == y, pp == p)

        @pl.when(here)
        def _():
            pltpu.make_async_copy(src, dst, recv).start()

        @pl.when(jnp.logical_not(here))
        def _():
            remote(src, dst, send, recv, tp, pp).start()

    def wait_bytes(like, sem):
        pltpu.make_async_copy(like, like, sem).wait()

    def own_parts(lo, hi):
        start = 0
        for ref in (qkv_ref, up_ref, wo_ref, down_ref):
            first, end = max(lo, start), min(hi, start + ref.shape[0])
            if first < end:
                yield ref.at[pl.ds(first - start, end - first)], pl.ds(first, end - first)
            start += ref.shape[0]

    @pl.when(home)
    def _():
        for i, ref in enumerate((ln_attn_ref, ln_mlp_ref)):
            pltpu.make_async_copy(ref, ln_s.at[i], ln_recv).start()
            remote(ref, ln_s.at[i], ln_send, ln_recv, y, sibling).start()
        for src, part in own_parts(0, 2 * half):
            pltpu.make_async_copy(src, wbuf.at[0, part], w_recv.at[0]).start()
            remote(src, wbuf.at[0, part], w_send.at[0], w_recv.at[0], y, sibling).start()

    pair_of_stage = (core + chip) % 2

    def send_x(i, carry):
        for b in range(ranks):
            put(stage_ref.at[b * blk + i], xs.at[0, i, my_seq], x_send, x_recv.at[0, i], 2 * pair_of_stage + b // 2, 2 * chip + b % 2)
        return carry

    lax.fori_loop(0, blk, send_x, 0)

    @pl.when(home)
    def _():
        for h in range(2):
            for src, part in own_parts(h * half, (h + 1) * half):
                remote(src, wbuf.at[1, part], w_send.at[1], w_recv.at[1], mate, 2 * chip + h).start()

    @pl.when(jnp.logical_not(home))
    def _():
        for h in range(2):
            for src, part in own_parts(h * half, (h + 1) * half):
                remote(src, wbuf.at[2, part], w_send.at[1], w_recv.at[3], across, 2 * chip + h).start()

    @pl.when(p == 0)
    def _():
        zero_s[...] = jnp.zeros_like(zero_s)

        def put_zero(n, carry):
            pltpu.make_async_copy(zero_s, final_ref.at[n], out_recv.at[0]).start()
            return carry

        lax.fori_loop(0, blk * ranks, put_zero, 0)

    mate_swap = [remote(wbuf.at[slot, my_half], wbuf.at[slot, my_half], w_send.at[1 + slot], w_recv.at[2 * slot], y, sibling) for slot in range(1, 4)]
    pass_on = remote(wbuf.at[2, my_half], wbuf.at[3, my_half], w_send.at[5], w_recv.at[5], mate, p)

    def before_slot(slot):
        if slot == 0:
            wait_bytes(ln_s, ln_recv)
            wait_bytes(wbuf.at[0], w_recv.at[0])
        elif slot == 1:
            wait_bytes(wbuf.at[2, my_half], w_recv.at[3])
            pass_on.start()
            mate_swap[1].start()
            wait_bytes(wbuf.at[1, my_half], w_recv.at[1])
            mate_swap[0].start()

            @pl.when(chip == 0)
            def _():
                def send_mb(i, carry):
                    for b in range(ranks // 2):
                        put(mb_ref.at[(2 * b + core) * blk + i], xs.at[1, i, my_seq], mb_send, x_recv.at[1, i], b, core)
                    return carry

                lax.fori_loop(0, blk, send_mb, 0)

            wait_bytes(wbuf.at[1, my_half], w_recv.at[2])
        elif slot == 2:
            wait_bytes(wbuf.at[2, my_half], w_recv.at[4])
        else:
            wait_bytes(wbuf.at[3, my_half], w_recv.at[5])
            mate_swap[2].start()
            wait_bytes(wbuf.at[3, my_half], w_recv.at[6])

    def send_emit(tick, dst, rows, row0, block):
        def body(n, carry):
            tp, pp = n // stages, n % stages
            src = xs.at[tick, pl.ds(row0, rows), pl.ds(pl.multiple_of(tp * seq_loc, seq_loc), seq_loc), pl.ds(pl.multiple_of(pp * cols, cols), cols)]
            put(src, dst.at[pl.ds(block * blk + row0, rows)], out_send, out_recv.at[1 + tick], tp, pp)
            return carry

        lax.fori_loop(0, ranks * stages, body, 0)

    steps = blk * ranks

    def step_body(step, carry):
        tick = step // steps
        index = step % steps
        slot = jnp.where(tick == 0, index // blk, index % ranks)
        row = jnp.where(tick == 0, index % blk, index // ranks)
        for s in range(ranks):
            @pl.when(step == s * blk)
            def _(s=s):
                before_slot(s)

        @pl.when(slot == 0)
        def _():
            wait_bytes(xs.at[tick, row], x_recv.at[tick, row])
            normalise(dims, xs.at[tick, row], acc.at[row], a_s.at[row], m_s.at[row], ln_s)

        add_quarter(dims, a_s.at[row], m_s.at[row], wbuf.at[slot], acc.at[row], cos_ref, sin_ref, q_s, k_s, v_s, o_s, h_s)

        @pl.when(slot == ranks - 1)
        def _():
            xs[tick, row] = acc[row].astype(BF16)

            @pl.when(jnp.logical_and(tick == 0, jnp.logical_not(last)))
            def _():
                next_y = jnp.where(role == 0, across, y)
                next_p = jnp.where(role == 0, p, p + 2)
                remote(xs.at[0, row], xs.at[1, row], y_send, x_recv.at[1, row], next_y, next_p).start()

            @pl.when(jnp.logical_and(step == steps - 1, last))
            def _():
                send_emit(0, emit_one, blk, 0, block_one)

            @pl.when(jnp.logical_and(tick == 1, last))
            def _():
                send_emit(1, emit_two, 1, row, block_two)

            @pl.when(jnp.logical_and(tick == 1, jnp.logical_not(last)))
            def _():
                def send_final(n, carry):
                    part = pl.ds(pl.multiple_of(n * seq_loc, seq_loc), seq_loc)
                    put(xs.at[1, row, part], final_ref.at[block_two * blk + row], out_send, out_recv.at[0], n, layer + 1)
                    return carry

                lax.fori_loop(0, ranks, send_final, 0)

        return carry

    lax.fori_loop(0, 2 * steps, step_body, 0)

    wait_bytes(stage_ref.at[pl.ds(0, (ranks - 1) * blk)], x_send)

    @pl.when(home)
    def _():
        wait_bytes(ln_s, ln_send)
        wait_bytes(wbuf.at[0], w_send.at[0])

    @pl.when(jnp.logical_not(home))
    def _():
        wait_bytes(stage_ref.at[pl.ds(0, blk)], x_send)

    wait_bytes(wbuf.at[0], w_send.at[1])
    for slot in range(2, 6):
        wait_bytes(wbuf.at[1, my_half], w_send.at[slot])

    @pl.when(chip == 0)
    def _():
        wait_bytes(mb_ref.at[pl.ds(0, blk)], mb_send)

        @pl.when(role == 1)
        def _():
            wait_bytes(mb_ref.at[pl.ds(0, blk)], mb_send)

    @pl.when(jnp.logical_not(last))
    def _():
        wait_bytes(xs.at[0], y_send)
        wait_bytes(xs.at[1, :, pl.ds(0, seq - seq_loc)], out_send)

        @pl.when(p != layer + 1)
        def _():
            wait_bytes(xs.at[1, :, pl.ds(0, seq_loc)], out_send)

    @pl.when(last)
    def _():
        wait_bytes(xs.at[:, :, pl.ds(0, seq - seq_loc)], out_send)
        wait_bytes(xs.at[:, :, pl.ds(0, seq_loc), pl.ds(0, width - cols)], out_send)

    wait_bytes(final_ref, out_recv.at[0])
    wait_bytes(emit_one, out_recv.at[1])
    wait_bytes(emit_two, out_recv.at[2])


def rope_tables(positions, head_dim):
    inv_freq = 1.0 / (ROPE_BASE ** (jnp.arange(0, head_dim, 2).astype(F32) / head_dim))
    angles = inv_freq[:, None] * positions.astype(F32)[None, :]
    return jnp.cos(angles), jnp.sin(angles)


def solution(mesh):
    stages = mesh.shape["pp"]
    ranks = mesh.shape["tp"]

    def stage_body(stage_buf, new_mb, positions, ln_attn, ln_mlp, w_qkv, w_out, w_up, w_down):
        mb, seq_loc, width = new_mb.shape
        seq = seq_loc * ranks
        blk = mb // ranks
        heads, head_dim = w_qkv.shape[1], w_qkv.shape[3]
        ff = w_up.shape[2]
        dims = (seq, width, heads, head_dim, ff)
        qk_w = heads * head_dim
        cos_tab, sin_tab = rope_tables(positions, head_dim)
        slot_rows = 4 * qk_w + width + ff
        hbm = pl.BlockSpec(memory_space=pltpu.HBM)
        vmem = pl.BlockSpec(memory_space=pltpu.VMEM)
        dma = pltpu.SemaphoreType.DMA
        emit = jax.ShapeDtypeStruct((mb, seq_loc, width // stages), BF16)
        emit_one, emit_two, final_buf = pl.pallas_call(
            functools.partial(ticks_kernel, dims, ranks, stages),
            out_shape=(emit, emit, jax.ShapeDtypeStruct((mb, seq_loc, width), BF16)),
            in_specs=[hbm] * 8 + [vmem] * 2,
            out_specs=(hbm, hbm, hbm),
            scratch_shapes=[
                pltpu.VMEM((ranks, slot_rows, width), BF16),
                pltpu.VMEM((2, blk, seq, width), BF16),
                pltpu.VMEM((blk, seq, width), F32),
                pltpu.VMEM((blk, seq, width), BF16),
                pltpu.VMEM((blk, seq, width), BF16),
                pltpu.VMEM((qk_w, seq), BF16),
                pltpu.VMEM((qk_w, seq), BF16),
                pltpu.VMEM((qk_w, seq), BF16),
                pltpu.VMEM((qk_w, seq), F32),
                pltpu.VMEM((seq, qk_w + ff), BF16),
                pltpu.VMEM((seq_loc, width), BF16),
                pltpu.VMEM((2, 2, width), F32),
                dma, dma((2, blk)), dma, dma((6,)), dma((7,)), dma, dma, dma((3,)), dma, dma,
            ],
            compiler_params=pltpu.CompilerParams(has_side_effects=True, vmem_limit_bytes=63 * 1000 * 1024),
        )(stage_buf[0], new_mb, w_qkv[0].reshape(3 * qk_w, width), w_up[0], w_out[0], w_down[0], ln_attn[0], ln_mlp[0], cos_tab, sin_tab)
        return emit_one, emit_two, final_buf[None]

    act_spec = P("dp", "tp", None)
    buf_spec = P("pp", "dp", "tp", None)
    emit_spec = P("dp", "tp", "pp")
    stack_spec = P("pp", None, None)
    return jax.shard_map(stage_body, mesh=mesh, in_specs=(buf_spec, act_spec, P(None), stack_spec, stack_spec, P("pp", "tp", None, None, None), P("pp", "tp", None), P("pp", None, "tp"), P("pp", "tp", None)), out_specs=(emit_spec, emit_spec, buf_spec), check_vma=False)
```

```python
import functools
import math

import jax
import jax.numpy as jnp
from jax import lax
from jax.experimental import pallas as pl
from jax.experimental.pallas import tpu as pltpu
from jax.sharding import PartitionSpec as P

LN_EPS = 1e-5
ROPE_BASE = 10000.0
F32 = jnp.float32
BF16 = jnp.bfloat16
MESH = pl.DeviceIdType.MESH
LN_ROWS = 64
Q_BLK = 256
HEAD_UNROLL = 4
COL = 256


def nt_dot(lhs, rhs):
    return lax.dot_general(lhs, rhs, (((1,), (1,)), ((), ())), preferred_element_type=F32)


def nn_dot(lhs, rhs):
    return jnp.dot(lhs, rhs, preferred_element_type=F32)


def tn_dot(lhs, rhs):
    return lax.dot_general(lhs, rhs, (((0,), (0,)), ((), ())), preferred_element_type=F32)


def gelu(pre):
    return 0.5 * pre * (1.0 + lax.erf(pre * math.sqrt(0.5)))


def normalise(dims, x_ref, acc_ref, a_ref, m_ref, ln_ref):
    def body(i, carry):
        rows = pl.ds(pl.multiple_of(i * LN_ROWS, LN_ROWS), LN_ROWS)
        wide = x_ref[rows, :].astype(F32)
        acc_ref[rows, :] = wide
        centered = wide - jnp.mean(wide, axis=-1, keepdims=True)
        var = jnp.mean(jnp.square(centered), axis=-1, keepdims=True)
        normed = centered * lax.rsqrt(var + LN_EPS)
        a_ref[rows, :] = (normed * ln_ref[0, 0:1, :] + ln_ref[0, 1:2, :]).astype(BF16)
        m_ref[rows, :] = (normed * ln_ref[1, 0:1, :] + ln_ref[1, 1:2, :]).astype(BF16)
        return carry

    lax.fori_loop(0, dims[0] // LN_ROWS, body, 0)


def add_quarter(dims, a_ref, m_ref, w, acc_ref, cos_ref, sin_ref, q_s, k_s, v_s, o_s, h_s):
    seq, width, heads, head_dim, ff = dims
    qk_w = heads * head_dim
    qkv_rows = 3 * qk_w
    hd2 = head_dim // 2
    qkv = nt_dot(w[0:qkv_rows, :], a_ref[...]).astype(BF16)
    cos = cos_ref[...]
    sin = sin_ref[...]
    for h in range(heads):
        base = 3 * h * head_dim
        for dst, lo in ((q_s, base), (k_s, base + head_dim)):
            first_half = qkv[lo:lo + hd2].astype(F32)
            second_half = qkv[lo + hd2:lo + head_dim].astype(F32)
            dst[h * head_dim:h * head_dim + hd2, :] = (first_half * cos - second_half * sin).astype(BF16)
            dst[h * head_dim + hd2:(h + 1) * head_dim, :] = (second_half * cos + first_half * sin).astype(BF16)
        v_s[h * head_dim:(h + 1) * head_dim, :] = qkv[base + 2 * head_dim:base + 3 * head_dim]

    exp_scale = math.log2(math.e) * head_dim ** -0.5
    causal = lax.broadcasted_iota(jnp.int32, (Q_BLK, Q_BLK), 0) <= lax.broadcasted_iota(jnp.int32, (Q_BLK, Q_BLK), 1)

    def head_body(h, carry):
        rows = pl.ds(pl.multiple_of(h * head_dim, head_dim), head_dim)
        for blk in range(seq // Q_BLK):
            lo = blk * Q_BLK
            hi = lo + Q_BLK
            query = q_s[rows, lo:hi]
            s_diag = jnp.where(causal, tn_dot(k_s[rows, lo:hi], query), -1e30)
            top = jnp.max(s_diag, axis=0, keepdims=True)
            if blk:
                s_past = tn_dot(k_s[rows, 0:lo], query)
                top = jnp.maximum(top, jnp.max(s_past, axis=0, keepdims=True))
            e_diag = jnp.exp2((s_diag - top) * exp_scale)
            tot = jnp.sum(e_diag, axis=0, keepdims=True)
            if blk:
                e_past = jnp.exp2((s_past - top) * exp_scale)
                tot = tot + jnp.sum(e_past, axis=0, keepdims=True)
            inv = 1.0 / tot
            o_blk = nn_dot(v_s[rows, lo:hi], (e_diag * inv).astype(BF16))
            if blk:
                o_blk = o_blk + nn_dot(v_s[rows, 0:lo], (e_past * inv).astype(BF16))
            o_s[rows, lo:hi] = o_blk
        return carry

    lax.fori_loop(0, heads, head_body, 0, unroll=HEAD_UNROLL)
    h_s[:, 0:qk_w] = jnp.transpose(o_s[...]).astype(BF16)

    for j in range(ff // COL):
        pre = nn_dot(m_ref[...], w[qkv_rows:qkv_rows + width, j * COL:(j + 1) * COL])
        h_s[:, qk_w + j * COL:qk_w + (j + 1) * COL] = gelu(pre).astype(BF16)
    out0 = qkv_rows + width
    for j in range(width // COL):
        acc_ref[:, j * COL:(j + 1) * COL] += nn_dot(h_s[...], w[out0:out0 + qk_w + ff, j * COL:(j + 1) * COL])


def ticks_kernel(dims, ranks, stages, stage_ref, mb_ref, qkv_ref, up_ref, wo_ref, down_ref, ln_attn_ref, ln_mlp_ref, cos_ref, sin_ref,
                 emit_one, emit_two, final_ref, wbuf, xs, acc, a_s, m_s, q_s, k_s, v_s, o_s, h_s, zero_s, ln_s, relay_s,
                 x_send, x_recv, mb_send, w_send, w_recv, y_send, out_send, out_recv, ln_send, ln_recv, relay_send, relay_recv):
    seq, width = dims[:2]
    seq_loc = seq // ranks
    blk = xs.shape[1]
    cols = width // stages
    half = wbuf.shape[1] // 2
    y = lax.axis_index("tp")
    p = lax.axis_index("pp")
    chip = p // 2
    core = p % 2
    role = (y // 2 + chip) % 2
    layer = 2 * chip + role
    last = layer == stages - 1
    home = core == role
    sibling = p + 1 - 2 * core
    mate = y + 1 - 2 * (y % 2)
    across = ranks - 1 - y
    block_one = 2 * (y % 2) + core
    block_two = jnp.where(role == 0, block_one, 2 * (1 - y % 2) + core)
    my_seq = pl.ds(pl.multiple_of(y * seq_loc, seq_loc), seq_loc)
    my_half = pl.ds(pl.multiple_of(core * half, half), half)

    def remote(src, dst, send, recv, tp, pp):
        return pltpu.make_async_remote_copy(src_ref=src, dst_ref=dst, send_sem=send, recv_sem=recv, device_id={"tp": tp, "pp": pp}, device_id_type=MESH)

    def put(src, dst, send, recv, tp, pp):
        here = jnp.logical_and(tp == y, pp == p)

        @pl.when(here)
        def _():
            pltpu.make_async_copy(src, dst, recv).start()

        @pl.when(jnp.logical_not(here))
        def _():
            remote(src, dst, send, recv, tp, pp).start()

    def wait_bytes(like, sem):
        pltpu.make_async_copy(like, like, sem).wait()

    def own_parts(lo, hi):
        start = 0
        for ref in (qkv_ref, up_ref, wo_ref, down_ref):
            first, end = max(lo, start), min(hi, start + ref.shape[0])
            if first < end:
                yield ref.at[pl.ds(first - start, end - first)], pl.ds(first, end - first)
            start += ref.shape[0]

    @pl.when(home)
    def _():
        for i, ref in enumerate((ln_attn_ref, ln_mlp_ref)):
            pltpu.make_async_copy(ref, ln_s.at[i], ln_recv).start()
            remote(ref, ln_s.at[i], ln_send, ln_recv, y, sibling).start()
        for src, part in own_parts(0, 2 * half):
            pltpu.make_async_copy(src, wbuf.at[0, part], w_recv.at[0]).start()
            remote(src, wbuf.at[0, part], w_send.at[0], w_recv.at[0], y, sibling).start()

    def x_part(block, i):
        return stage_ref.at[block * blk + i]

    def send_home(i):
        for b in range(2):
            remote(x_part(2 * (mate % 2) + b, i), xs.at[0, i, my_seq], x_send, x_recv.at[0, i], mate, 2 * chip + b).start()

    def relay(i):
        wait_bytes(relay_s.at[pl.ds(2 * i, 2)], relay_recv.at[i])
        seq_across = pl.ds(pl.multiple_of(across * seq_loc, seq_loc), seq_loc)
        for b in range(2):
            remote(relay_s.at[2 * i + b], xs.at[0, i, seq_across], relay_send, x_recv.at[0, i], mate, 2 * chip + b).start()

    @pl.when(home)
    def _():
        def keep(i, carry):
            pltpu.make_async_copy(x_part(2 * (y % 2) + core, i), xs.at[0, i, my_seq], x_recv.at[0, i]).start()
            remote(x_part(2 * (y % 2) + 1 - core, i), xs.at[0, i, my_seq], x_send, x_recv.at[0, i], y, sibling).start()
            return carry

        lax.fori_loop(0, blk, keep, 0)
        for i in range(2):
            send_home(i)

    @pl.when(jnp.logical_not(home))
    def _():
        def send_across(i, carry):
            for b in range(2):
                remote(x_part(2 * (1 - across % 2) + b, i), relay_s.at[2 * i + b], x_send, relay_recv.at[i], across, p).start()
            for b in range(2):
                remote(x_part(2 * (across % 2) + b, i), xs.at[0, i, my_seq], x_send, x_recv.at[0, i], across, 2 * chip + b).start()
            return carry

        lax.fori_loop(0, blk, send_across, 0)
        for h in range(2):
            for src, part in own_parts(h * half, (h + 1) * half):
                remote(src, wbuf.at[2, part], w_send.at[1], w_recv.at[3], across, 2 * chip + h).start()

    def relay_step(i):
        @pl.when(home)
        def _():
            relay(i)
            if i + 2 < blk:
                send_home(i + 2)
            if i == blk - 1:
                for h in range(2):
                    for src, part in own_parts(h * half, (h + 1) * half):
                        remote(src, wbuf.at[1, part], w_send.at[1], w_recv.at[1], mate, 2 * chip + h).start()

    @pl.when(p == 0)
    def _():
        zero_s[...] = jnp.zeros_like(zero_s)

        def put_zero(n, carry):
            pltpu.make_async_copy(zero_s, final_ref.at[n], out_recv.at[0]).start()
            return carry

        lax.fori_loop(0, blk * ranks, put_zero, 0)

    mate_swap = [remote(wbuf.at[slot, my_half], wbuf.at[slot, my_half], w_send.at[1 + slot], w_recv.at[2 * slot], y, sibling) for slot in range(1, 4)]
    pass_on = remote(wbuf.at[2, my_half], wbuf.at[3, my_half], w_send.at[5], w_recv.at[5], mate, p)

    def before_slot(slot):
        if slot == 0:
            wait_bytes(ln_s, ln_recv)
            wait_bytes(wbuf.at[0], w_recv.at[0])
        elif slot == 1:
            wait_bytes(wbuf.at[2, my_half], w_recv.at[3])
            pass_on.start()
            mate_swap[1].start()
            wait_bytes(wbuf.at[1, my_half], w_recv.at[1])
            mate_swap[0].start()

            wait_bytes(wbuf.at[1, my_half], w_recv.at[2])
        elif slot == 2:
            wait_bytes(wbuf.at[2, my_half], w_recv.at[4])
        else:
            wait_bytes(wbuf.at[3, my_half], w_recv.at[5])
            mate_swap[2].start()

            @pl.when(chip == 0)
            def _():
                def send_mb(i, carry):
                    for b in range(ranks // 2):
                        put(mb_ref.at[(2 * b + core) * blk + i], xs.at[1, i, my_seq], mb_send, x_recv.at[1, i], b, core)
                    return carry

                lax.fori_loop(0, blk, send_mb, 0)

            wait_bytes(wbuf.at[3, my_half], w_recv.at[6])

    def send_emit(tick, dst, rows, row0, block):
        def body(n, carry):
            tp, pp = n // stages, n % stages
            src = xs.at[tick, pl.ds(row0, rows), pl.ds(pl.multiple_of(tp * seq_loc, seq_loc), seq_loc), pl.ds(pl.multiple_of(pp * cols, cols), cols)]
            put(src, dst.at[pl.ds(block * blk + row0, rows)], out_send, out_recv.at[1 + tick], tp, pp)
            return carry

        lax.fori_loop(0, ranks * stages, body, 0)

    steps = blk * ranks

    def step_body(step, carry):
        tick = step // steps
        index = step % steps
        slot = jnp.where(tick == 0, index // blk, index % ranks)
        row = jnp.where(tick == 0, index % blk, index // ranks)
        for s in range(ranks):
            @pl.when(step == s * blk)
            def _(s=s):
                before_slot(s)

        for i in range(blk):
            @pl.when(step == i)
            def _(i=i):
                relay_step(i)

        @pl.when(slot == 0)
        def _():
            wait_bytes(xs.at[tick, row], x_recv.at[tick, row])
            normalise(dims, xs.at[tick, row], acc.at[row], a_s.at[row], m_s.at[row], ln_s)

        add_quarter(dims, a_s.at[row], m_s.at[row], wbuf.at[slot], acc.at[row], cos_ref, sin_ref, q_s, k_s, v_s, o_s, h_s)

        @pl.when(slot == ranks - 1)
        def _():
            xs[tick, row] = acc[row].astype(BF16)

            @pl.when(jnp.logical_and(tick == 0, jnp.logical_not(last)))
            def _():
                next_y = jnp.where(role == 0, across, y)
                next_p = jnp.where(role == 0, p, p + 2)
                remote(xs.at[0, row], xs.at[1, row], y_send, x_recv.at[1, row], next_y, next_p).start()

            @pl.when(jnp.logical_and(step == steps - 1, last))
            def _():
                send_emit(0, emit_one, blk, 0, block_one)

            @pl.when(jnp.logical_and(tick == 1, last))
            def _():
                send_emit(1, emit_two, 1, row, block_two)

            @pl.when(jnp.logical_and(tick == 1, jnp.logical_not(last)))
            def _():
                def send_final(n, carry):
                    part = pl.ds(pl.multiple_of(n * seq_loc, seq_loc), seq_loc)
                    put(xs.at[1, row, part], final_ref.at[block_two * blk + row], out_send, out_recv.at[0], n, layer + 1)
                    return carry

                lax.fori_loop(0, ranks, send_final, 0)

        return carry

    lax.fori_loop(0, 2 * steps, step_body, 0)

    wait_bytes(stage_ref.at[pl.ds(0, (ranks - 1) * blk)], x_send)

    @pl.when(home)
    def _():
        wait_bytes(ln_s, ln_send)
        wait_bytes(relay_s, relay_send)
        wait_bytes(wbuf.at[0], w_send.at[0])

    @pl.when(jnp.logical_not(home))
    def _():
        wait_bytes(stage_ref.at[pl.ds(0, blk)], x_send)

    wait_bytes(wbuf.at[0], w_send.at[1])
    for slot in range(2, 6):
        wait_bytes(wbuf.at[1, my_half], w_send.at[slot])

    @pl.when(chip == 0)
    def _():
        wait_bytes(mb_ref.at[pl.ds(0, blk)], mb_send)

        @pl.when(role == 1)
        def _():
            wait_bytes(mb_ref.at[pl.ds(0, blk)], mb_send)

    @pl.when(jnp.logical_not(last))
    def _():
        wait_bytes(xs.at[0], y_send)
        wait_bytes(xs.at[1, :, pl.ds(0, seq - seq_loc)], out_send)

        @pl.when(p != layer + 1)
        def _():
            wait_bytes(xs.at[1, :, pl.ds(0, seq_loc)], out_send)

    @pl.when(last)
    def _():
        wait_bytes(xs.at[:, :, pl.ds(0, seq - seq_loc)], out_send)
        wait_bytes(xs.at[:, :, pl.ds(0, seq_loc), pl.ds(0, width - cols)], out_send)

    wait_bytes(final_ref, out_recv.at[0])
    wait_bytes(emit_one, out_recv.at[1])
    wait_bytes(emit_two, out_recv.at[2])


def rope_tables(positions, head_dim):
    inv_freq = 1.0 / (ROPE_BASE ** (jnp.arange(0, head_dim, 2).astype(F32) / head_dim))
    angles = inv_freq[:, None] * positions.astype(F32)[None, :]
    return jnp.cos(angles), jnp.sin(angles)


def solution(mesh):
    stages = mesh.shape["pp"]
    ranks = mesh.shape["tp"]

    def stage_body(stage_buf, new_mb, positions, ln_attn, ln_mlp, w_qkv, w_out, w_up, w_down):
        mb, seq_loc, width = new_mb.shape
        seq = seq_loc * ranks
        blk = mb // ranks
        heads, head_dim = w_qkv.shape[1], w_qkv.shape[3]
        ff = w_up.shape[2]
        dims = (seq, width, heads, head_dim, ff)
        qk_w = heads * head_dim
        cos_tab, sin_tab = rope_tables(positions, head_dim)
        slot_rows = 4 * qk_w + width + ff
        hbm = pl.BlockSpec(memory_space=pltpu.HBM)
        vmem = pl.BlockSpec(memory_space=pltpu.VMEM)
        dma = pltpu.SemaphoreType.DMA
        emit = jax.ShapeDtypeStruct((mb, seq_loc, width // stages), BF16)
        emit_one, emit_two, final_buf = pl.pallas_call(
            functools.partial(ticks_kernel, dims, ranks, stages),
            out_shape=(emit, emit, jax.ShapeDtypeStruct((mb, seq_loc, width), BF16)),
            in_specs=[hbm] * 8 + [vmem] * 2,
            out_specs=(hbm, hbm, hbm),
            scratch_shapes=[
                pltpu.VMEM((ranks, slot_rows, width), BF16),
                pltpu.VMEM((2, blk, seq, width), BF16),
                pltpu.VMEM((blk, seq, width), F32),
                pltpu.VMEM((blk, seq, width), BF16),
                pltpu.VMEM((blk, seq, width), BF16),
                pltpu.VMEM((qk_w, seq), BF16),
                pltpu.VMEM((qk_w, seq), BF16),
                pltpu.VMEM((qk_w, seq), BF16),
                pltpu.VMEM((qk_w, seq), F32),
                pltpu.VMEM((seq, qk_w + ff), BF16),
                pltpu.VMEM((seq_loc, width), BF16),
                pltpu.VMEM((2, 2, width), F32),
                pltpu.VMEM((2 * blk, seq_loc, width), BF16),
                dma, dma((2, blk)), dma, dma((6,)), dma((7,)), dma, dma, dma((3,)), dma, dma, dma, dma((blk,)),
            ],
            compiler_params=pltpu.CompilerParams(has_side_effects=True, vmem_limit_bytes=63 * 1000 * 1024),
        )(stage_buf[0], new_mb, w_qkv[0].reshape(3 * qk_w, width), w_up[0], w_out[0], w_down[0], ln_attn[0], ln_mlp[0], cos_tab, sin_tab)
        return emit_one, emit_two, final_buf[None]

    act_spec = P("dp", "tp", None)
    buf_spec = P("pp", "dp", "tp", None)
    emit_spec = P("dp", "tp", "pp")
    stack_spec = P("pp", None, None)
    return jax.shard_map(stage_body, mesh=mesh, in_specs=(buf_spec, act_spec, P(None), stack_spec, stack_spec, P("pp", "tp", None, None, None), P("pp", "tp", None), P("pp", None, "tp"), P("pp", "tp", None)), out_specs=(emit_spec, emit_spec, buf_spec), check_vma=False)
```

```python
import functools
import math

import jax
import jax.numpy as jnp
from jax import lax
from jax.experimental import pallas as pl
from jax.experimental.pallas import tpu as pltpu
from jax.sharding import PartitionSpec as P

LN_EPS = 1e-5
ROPE_BASE = 10000.0
F32 = jnp.float32
BF16 = jnp.bfloat16
MESH = pl.DeviceIdType.MESH
LN_ROWS = 64
Q_BLK = 256
HEAD_UNROLL = 4
COL = 256


def nt_dot(lhs, rhs):
    return lax.dot_general(lhs, rhs, (((1,), (1,)), ((), ())), preferred_element_type=F32)


def nn_dot(lhs, rhs):
    return jnp.dot(lhs, rhs, preferred_element_type=F32)


def tn_dot(lhs, rhs):
    return lax.dot_general(lhs, rhs, (((0,), (0,)), ((), ())), preferred_element_type=F32)


def gelu(pre):
    return 0.5 * pre * (1.0 + lax.erf(pre * math.sqrt(0.5)))


def normalise(dims, x_ref, acc_ref, a_ref, m_ref, ln_ref):
    def body(i, carry):
        rows = pl.ds(pl.multiple_of(i * LN_ROWS, LN_ROWS), LN_ROWS)
        wide = x_ref[rows, :].astype(F32)
        acc_ref[rows, :] = wide
        centered = wide - jnp.mean(wide, axis=-1, keepdims=True)
        var = jnp.mean(jnp.square(centered), axis=-1, keepdims=True)
        normed = centered * lax.rsqrt(var + LN_EPS)
        a_ref[rows, :] = (normed * ln_ref[0, 0:1, :] + ln_ref[0, 1:2, :]).astype(BF16)
        m_ref[rows, :] = (normed * ln_ref[1, 0:1, :] + ln_ref[1, 1:2, :]).astype(BF16)
        return carry

    lax.fori_loop(0, dims[0] // LN_ROWS, body, 0)


def add_quarter(dims, a_ref, m_ref, w, acc_ref, cos_ref, sin_ref, q_s, k_s, v_s, o_s, h_s):
    seq, width, heads, head_dim, ff = dims
    qk_w = heads * head_dim
    qkv_rows = 3 * qk_w
    hd2 = head_dim // 2
    qkv = nt_dot(w[0:qkv_rows, :], a_ref[...]).astype(BF16)
    cos = cos_ref[...]
    sin = sin_ref[...]
    for h in range(heads):
        base = 3 * h * head_dim
        for dst, lo in ((q_s, base), (k_s, base + head_dim)):
            first_half = qkv[lo:lo + hd2].astype(F32)
            second_half = qkv[lo + hd2:lo + head_dim].astype(F32)
            dst[h * head_dim:h * head_dim + hd2, :] = (first_half * cos - second_half * sin).astype(BF16)
            dst[h * head_dim + hd2:(h + 1) * head_dim, :] = (second_half * cos + first_half * sin).astype(BF16)
        v_s[h * head_dim:(h + 1) * head_dim, :] = qkv[base + 2 * head_dim:base + 3 * head_dim]

    exp_scale = math.log2(math.e) * head_dim ** -0.5
    causal = lax.broadcasted_iota(jnp.int32, (Q_BLK, Q_BLK), 0) <= lax.broadcasted_iota(jnp.int32, (Q_BLK, Q_BLK), 1)

    def head_body(h, carry):
        rows = pl.ds(pl.multiple_of(h * head_dim, head_dim), head_dim)
        for blk in range(seq // Q_BLK):
            lo = blk * Q_BLK
            hi = lo + Q_BLK
            query = q_s[rows, lo:hi]
            s_diag = jnp.where(causal, tn_dot(k_s[rows, lo:hi], query), -1e30)
            top = jnp.max(s_diag, axis=0, keepdims=True)
            if blk:
                s_past = tn_dot(k_s[rows, 0:lo], query)
                top = jnp.maximum(top, jnp.max(s_past, axis=0, keepdims=True))
            e_diag = jnp.exp2((s_diag - top) * exp_scale)
            tot = jnp.sum(e_diag, axis=0, keepdims=True)
            if blk:
                e_past = jnp.exp2((s_past - top) * exp_scale)
                tot = tot + jnp.sum(e_past, axis=0, keepdims=True)
            inv = 1.0 / tot
            o_blk = nn_dot(v_s[rows, lo:hi], (e_diag * inv).astype(BF16))
            if blk:
                o_blk = o_blk + nn_dot(v_s[rows, 0:lo], (e_past * inv).astype(BF16))
            o_s[rows, lo:hi] = o_blk
        return carry

    lax.fori_loop(0, heads, head_body, 0, unroll=HEAD_UNROLL)
    h_s[:, 0:qk_w] = jnp.transpose(o_s[...]).astype(BF16)

    for j in range(ff // COL):
        pre = nn_dot(m_ref[...], w[qkv_rows:qkv_rows + width, j * COL:(j + 1) * COL])
        h_s[:, qk_w + j * COL:qk_w + (j + 1) * COL] = gelu(pre).astype(BF16)
    out0 = qkv_rows + width
    for j in range(width // COL):
        acc_ref[:, j * COL:(j + 1) * COL] += nn_dot(h_s[...], w[out0:out0 + qk_w + ff, j * COL:(j + 1) * COL])


def ticks_kernel(dims, ranks, stages, stage_ref, mb_ref, qkv_ref, up_ref, wo_ref, down_ref, ln_attn_ref, ln_mlp_ref, cos_ref, sin_ref,
                 emit_one, emit_two, final_ref, wbuf, xs, acc, a_s, m_s, q_s, k_s, v_s, o_s, h_s, zero_s, ln_s,
                 x_send, x_recv, mb_send, w_send, w_recv, y_send, out_send, out_recv, ln_send, ln_recv):
    seq, width = dims[:2]
    seq_loc = seq // ranks
    blk = xs.shape[1]
    cols = width // stages
    half = wbuf.shape[1] // 2
    y = lax.axis_index("tp")
    p = lax.axis_index("pp")
    chip = p // 2
    core = p % 2
    role = (y // 2 + chip) % 2
    layer = 2 * chip + role
    last = layer == stages - 1
    home = core == role
    sibling = p + 1 - 2 * core
    mate = y + 1 - 2 * (y % 2)
    across = ranks - 1 - y
    block_one = 2 * (y % 2) + core
    block_two = jnp.where(role == 0, block_one, 2 * (1 - y % 2) + core)
    my_seq = pl.ds(pl.multiple_of(y * seq_loc, seq_loc), seq_loc)
    my_half = pl.ds(pl.multiple_of(core * half, half), half)

    def remote(src, dst, send, recv, tp, pp):
        return pltpu.make_async_remote_copy(src_ref=src, dst_ref=dst, send_sem=send, recv_sem=recv, device_id={"tp": tp, "pp": pp}, device_id_type=MESH)

    def put(src, dst, send, recv, tp, pp):
        here = jnp.logical_and(tp == y, pp == p)

        @pl.when(here)
        def _():
            pltpu.make_async_copy(src, dst, recv).start()

        @pl.when(jnp.logical_not(here))
        def _():
            remote(src, dst, send, recv, tp, pp).start()

    def wait_bytes(like, sem):
        pltpu.make_async_copy(like, like, sem).wait()

    def own_parts(lo, hi):
        start = 0
        for ref in (qkv_ref, up_ref, wo_ref, down_ref):
            first, end = max(lo, start), min(hi, start + ref.shape[0])
            if first < end:
                yield ref.at[pl.ds(first - start, end - first)], pl.ds(first, end - first)
            start += ref.shape[0]

    @pl.when(home)
    def _():
        for i, ref in enumerate((ln_attn_ref, ln_mlp_ref)):
            pltpu.make_async_copy(ref, ln_s.at[i], ln_recv).start()
            remote(ref, ln_s.at[i], ln_send, ln_recv, y, sibling).start()
        for src, part in own_parts(0, 2 * half):
            pltpu.make_async_copy(src, wbuf.at[0, part], w_recv.at[0]).start()
            remote(src, wbuf.at[0, part], w_send.at[0], w_recv.at[0], y, sibling).start()

    pair_of_stage = (core + chip) % 2

    def send_x(i, carry):
        for b in range(ranks):
            put(stage_ref.at[b * blk + i], xs.at[0, i, my_seq], x_send, x_recv.at[0, i], 2 * pair_of_stage + b // 2, 2 * chip + b % 2)
        return carry

    lax.fori_loop(0, blk, send_x, 0)

    @pl.when(home)
    def _():
        for h in range(2):
            for src, part in own_parts(h * half, (h + 1) * half):
                remote(src, wbuf.at[1, part], w_send.at[1], w_recv.at[1], mate, 2 * chip + h).start()

    @pl.when(jnp.logical_not(home))
    def _():
        for h in range(2):
            for src, part in own_parts(h * half, (h + 1) * half):
                remote(src, wbuf.at[2, part], w_send.at[1], w_recv.at[3], across, 2 * chip + h).start()

    @pl.when(p == 0)
    def _():
        zero_s[...] = jnp.zeros_like(zero_s)

        def put_zero(n, carry):
            pltpu.make_async_copy(zero_s, final_ref.at[n], out_recv.at[0]).start()
            return carry

        lax.fori_loop(0, blk * ranks, put_zero, 0)

    mate_swap = [remote(wbuf.at[slot, my_half], wbuf.at[slot, my_half], w_send.at[1 + slot], w_recv.at[2 * slot], y, sibling) for slot in range(1, 4)]
    pass_on = remote(wbuf.at[2, my_half], wbuf.at[3, my_half], w_send.at[5], w_recv.at[5], mate, p)

    def before_slot(slot):
        if slot == 0:
            wait_bytes(ln_s, ln_recv)
            wait_bytes(wbuf.at[0], w_recv.at[0])
        elif slot == 1:
            wait_bytes(wbuf.at[1, my_half], w_recv.at[1])
            mate_swap[0].start()
            wait_bytes(wbuf.at[1, my_half], w_recv.at[2])
        elif slot == 2:
            wait_bytes(wbuf.at[2, my_half], w_recv.at[4])
        else:
            wait_bytes(wbuf.at[3, my_half], w_recv.at[5])
            mate_swap[2].start()
            wait_bytes(wbuf.at[3, my_half], w_recv.at[6])

    def send_emit(tick, dst, rows, row0, block):
        def body(n, carry):
            tp, pp = n // stages, n % stages
            src = xs.at[tick, pl.ds(row0, rows), pl.ds(pl.multiple_of(tp * seq_loc, seq_loc), seq_loc), pl.ds(pl.multiple_of(pp * cols, cols), cols)]
            put(src, dst.at[pl.ds(block * blk + row0, rows)], out_send, out_recv.at[1 + tick], tp, pp)
            return carry

        lax.fori_loop(0, ranks * stages, body, 0)

    steps = blk * ranks

    def step_body(step, carry):
        tick = step // steps
        index = step % steps
        slot = jnp.where(tick == 0, index // blk, index % ranks)
        row = jnp.where(tick == 0, index % blk, index // ranks)
        for s in range(ranks):
            @pl.when(step == s * blk)
            def _(s=s):
                before_slot(s)

        @pl.when(step == blk + blk // 2)
        def _():
            wait_bytes(wbuf.at[2, my_half], w_recv.at[3])
            pass_on.start()
            mate_swap[1].start()

            @pl.when(chip == 0)
            def _():
                def send_mb(i, carry):
                    for b in range(ranks // 2):
                        put(mb_ref.at[(2 * b + core) * blk + i], xs.at[1, i, my_seq], mb_send, x_recv.at[1, i], b, core)
                    return carry

                lax.fori_loop(0, blk, send_mb, 0)

        @pl.when(slot == 0)
        def _():
            wait_bytes(xs.at[tick, row], x_recv.at[tick, row])
            normalise(dims, xs.at[tick, row], acc.at[row], a_s.at[row], m_s.at[row], ln_s)

        add_quarter(dims, a_s.at[row], m_s.at[row], wbuf.at[slot], acc.at[row], cos_ref, sin_ref, q_s, k_s, v_s, o_s, h_s)

        @pl.when(slot == ranks - 1)
        def _():
            xs[tick, row] = acc[row].astype(BF16)

            @pl.when(jnp.logical_and(tick == 0, jnp.logical_not(last)))
            def _():
                next_y = jnp.where(role == 0, across, y)
                next_p = jnp.where(role == 0, p, p + 2)
                remote(xs.at[0, row], xs.at[1, row], y_send, x_recv.at[1, row], next_y, next_p).start()

            @pl.when(jnp.logical_and(step == steps + 2 * ranks - 1, last))
            def _():
                send_emit(0, emit_one, blk, 0, block_one)

            @pl.when(jnp.logical_and(tick == 1, last))
            def _():
                send_emit(1, emit_two, 1, row, block_two)

            @pl.when(jnp.logical_and(tick == 1, jnp.logical_not(last)))
            def _():
                def send_final(n, carry):
                    part = pl.ds(pl.multiple_of(n * seq_loc, seq_loc), seq_loc)
                    put(xs.at[1, row, part], final_ref.at[block_two * blk + row], out_send, out_recv.at[0], n, layer + 1)
                    return carry

                lax.fori_loop(0, ranks, send_final, 0)

        return carry

    lax.fori_loop(0, 2 * steps, step_body, 0)

    wait_bytes(stage_ref.at[pl.ds(0, (ranks - 1) * blk)], x_send)

    @pl.when(home)
    def _():
        wait_bytes(ln_s, ln_send)
        wait_bytes(wbuf.at[0], w_send.at[0])

    @pl.when(jnp.logical_not(home))
    def _():
        wait_bytes(stage_ref.at[pl.ds(0, blk)], x_send)

    wait_bytes(wbuf.at[0], w_send.at[1])
    for slot in range(2, 6):
        wait_bytes(wbuf.at[1, my_half], w_send.at[slot])

    @pl.when(chip == 0)
    def _():
        wait_bytes(mb_ref.at[pl.ds(0, blk)], mb_send)

        @pl.when(role == 1)
        def _():
            wait_bytes(mb_ref.at[pl.ds(0, blk)], mb_send)

    @pl.when(jnp.logical_not(last))
    def _():
        wait_bytes(xs.at[0], y_send)
        wait_bytes(xs.at[1, :, pl.ds(0, seq - seq_loc)], out_send)

        @pl.when(p != layer + 1)
        def _():
            wait_bytes(xs.at[1, :, pl.ds(0, seq_loc)], out_send)

    @pl.when(last)
    def _():
        wait_bytes(xs.at[:, :, pl.ds(0, seq - seq_loc)], out_send)
        wait_bytes(xs.at[:, :, pl.ds(0, seq_loc), pl.ds(0, width - cols)], out_send)

    wait_bytes(final_ref, out_recv.at[0])
    wait_bytes(emit_one, out_recv.at[1])
    wait_bytes(emit_two, out_recv.at[2])


def rope_tables(positions, head_dim):
    inv_freq = 1.0 / (ROPE_BASE ** (jnp.arange(0, head_dim, 2).astype(F32) / head_dim))
    angles = inv_freq[:, None] * positions.astype(F32)[None, :]
    return jnp.cos(angles), jnp.sin(angles)


def solution(mesh):
    stages = mesh.shape["pp"]
    ranks = mesh.shape["tp"]

    def stage_body(stage_buf, new_mb, positions, ln_attn, ln_mlp, w_qkv, w_out, w_up, w_down):
        mb, seq_loc, width = new_mb.shape
        seq = seq_loc * ranks
        blk = mb // ranks
        heads, head_dim = w_qkv.shape[1], w_qkv.shape[3]
        ff = w_up.shape[2]
        dims = (seq, width, heads, head_dim, ff)
        qk_w = heads * head_dim
        cos_tab, sin_tab = rope_tables(positions, head_dim)
        slot_rows = 4 * qk_w + width + ff
        hbm = pl.BlockSpec(memory_space=pltpu.HBM)
        vmem = pl.BlockSpec(memory_space=pltpu.VMEM)
        dma = pltpu.SemaphoreType.DMA
        emit = jax.ShapeDtypeStruct((mb, seq_loc, width // stages), BF16)
        emit_one, emit_two, final_buf = pl.pallas_call(
            functools.partial(ticks_kernel, dims, ranks, stages),
            out_shape=(emit, emit, jax.ShapeDtypeStruct((mb, seq_loc, width), BF16)),
            in_specs=[hbm] * 8 + [vmem] * 2,
            out_specs=(hbm, hbm, hbm),
            scratch_shapes=[
                pltpu.VMEM((ranks, slot_rows, width), BF16),
                pltpu.VMEM((2, blk, seq, width), BF16),
                pltpu.VMEM((blk, seq, width), F32),
                pltpu.VMEM((blk, seq, width), BF16),
                pltpu.VMEM((blk, seq, width), BF16),
                pltpu.VMEM((qk_w, seq), BF16),
                pltpu.VMEM((qk_w, seq), BF16),
                pltpu.VMEM((qk_w, seq), BF16),
                pltpu.VMEM((qk_w, seq), F32),
                pltpu.VMEM((seq, qk_w + ff), BF16),
                pltpu.VMEM((seq_loc, width), BF16),
                pltpu.VMEM((2, 2, width), F32),
                dma, dma((2, blk)), dma, dma((6,)), dma((7,)), dma, dma, dma((3,)), dma, dma,
            ],
            compiler_params=pltpu.CompilerParams(has_side_effects=True, vmem_limit_bytes=63 * 1000 * 1024),
        )(stage_buf[0], new_mb, w_qkv[0].reshape(3 * qk_w, width), w_up[0], w_out[0], w_down[0], ln_attn[0], ln_mlp[0], cos_tab, sin_tab)
        return emit_one, emit_two, final_buf[None]

    act_spec = P("dp", "tp", None)
    buf_spec = P("pp", "dp", "tp", None)
    emit_spec = P("dp", "tp", "pp")
    stack_spec = P("pp", None, None)
    return jax.shard_map(stage_body, mesh=mesh, in_specs=(buf_spec, act_spec, P(None), stack_spec, stack_spec, P("pp", "tp", None, None, None), P("pp", "tp", None), P("pp", None, "tp"), P("pp", "tp", None)), out_specs=(emit_spec, emit_spec, buf_spec), check_vma=False)
```
